32 devices in a mesh: gx: 2 (over x), gy: 4 (over y, core), gz: 4 (over z).
Axes of the slice: x: 2, y: 2, z: 4, core: 2. Of those that a mesh axis runs over, the one named last changes fastest.
Arguments:
- dual_rhs: float32 [2, 4, 4, 3, 300, 128], P('gx', 'gy', 'gz'), may hold values from -6 to 6
- local_flex: bfloat16 [2, 4, 4, 1800, 1800], P('gx', 'gy', 'gz'), as said below
- corner_coupling: bfloat16 [2, 4, 4, 24, 1800], P('gx', 'gy', 'gz'), may hold values from -0.375 to 0.375
- face_stiffness: bfloat16 [2, 4, 4, 6, 300, 300], P('gx', 'gy', 'gz'), as said below
- coarse_inverse: bfloat16 [27, 27], replicated, as said below
- corner_ids: int32 [2, 4, 4, 8], P('gx', 'gy', 'gz'), may hold values from -1 to 8, as said below
Outputs:
- multipliers: float32 [2, 4, 4, 3, 300, 128], P('gx', 'gy', 'gz')
- residual: float32 [2, 4, 4, 3, 300, 128], P('gx', 'gy', 'gz')
The draws below stay inside these ranges and needn't reach their ends.
Inputs may be any that keep to these rules, and one draw needn't show every extreme that they name: `local_flex`: each subdomain's matrix is symmetric positive definite. `face_stiffness`: each face block is symmetric positive definite. `coarse_inverse`: symmetric positive definite. `corner_ids`: entry k = 4 kx + 2 ky + kz of subdomain (i, j, l) is the number of the corner at lattice point (i + kx, j + ky, l + kz) when that point has all coordinates strictly between 0 and the subdomain counts, else -1; the 9 interior corners are numbered by a permutation, so subdomains sharing a corner name the same node.
All inputs are finite; a program needn't handle non-finite values.
Results may differ from the reference program's by a relative error of at most 0.04.
Values may be sent and summed in bfloat16 or wider, within the bound.
A program may use at most 64 MiB of HBM per device.

```python
import math
import jax
import jax.numpy as jnp
from jax import lax

P_SIZE = 300
R = 128
ITERS = 3
SX = 2
SY = 4
SZ = 4
Q = 1800
NNODE = 9
NC = 27


def spd_block(block_key, order, lowest, highest, spread):
    first, second = jax.random.split(block_key, 2)
    diagonal = jax.random.uniform(first, (order,), jnp.float32, lowest, highest)
    gaussian = jax.random.normal(second, (order, order), jnp.float32)
    matrix = (gaussian + gaussian.T) * (spread / math.sqrt(2.0 * order)) + jnp.diag(diagonal)
    return matrix


def draw_local_flex(key, part):
    base_key = jax.random.fold_in(key, 11)

    def one_block(block_index):
        return spd_block(jax.random.fold_in(base_key, block_index), Q, 0.7, 1.8, 0.28).astype(jnp.bfloat16)
    matrices = lax.map(one_block, jnp.arange(SX * SY * SZ))
    return matrices.reshape(SX, SY, SZ, Q, Q)


def draw_face_stiffness(key, part):
    base_key = jax.random.fold_in(key, 23)

    def one_block(block_index):
        return spd_block(jax.random.fold_in(base_key, block_index), P_SIZE, 1.0, 2.5, 0.4).astype(jnp.bfloat16)
    matrices = lax.map(one_block, jnp.arange(SX * SY * SZ * 6))
    return matrices.reshape(SX, SY, SZ, 6, P_SIZE, P_SIZE)


def draw_coarse_inverse(key, part):
    return spd_block(jax.random.fold_in(key, 37), NC, 0.6, 1.4, 0.24).astype(jnp.bfloat16)


def draw_corner_ids(key, part):
    numbering = jax.random.permutation(jax.random.fold_in(key, 53), NNODE).astype(jnp.int32)
    corner = jnp.arange(8, dtype=jnp.int32)
    point_x = jnp.arange(SX, dtype=jnp.int32)[:, None, None, None] + corner // 4
    point_y = jnp.arange(SY, dtype=jnp.int32)[None, :, None, None] + corner // 2 % 2
    point_z = jnp.arange(SZ, dtype=jnp.int32)[None, None, :, None] + corner % 2
    inside = (point_x >= 1) & (point_x <= SX - 1) & (point_y >= 1) & (point_y <= SY - 1) & (point_z >= 1) & (point_z <= SZ - 1)
    lattice_index = ((point_x - 1) * (SY - 1) + (point_y - 1)) * (SZ - 1) + (point_z - 1)
    lattice_index = jnp.where(inside, lattice_index, 0)
    return jnp.where(inside, numbering[lattice_index], -1).astype(jnp.int32)


def level_of(rng, shape, cuts, low, top_value):
    factor_of, own = 1.0, jax.random.fold_in(rng, 6)
    for dim, parts in cuts:
        steps = jnp.exp(jax.random.uniform(jax.random.fold_in(own, dim), (parts,), jnp.float32, low / len(cuts), top_value / len(cuts)))
        factor_of = factor_of * jnp.repeat(steps, shape[dim] // parts).reshape([-1 if axis == dim else 1 for axis in range(len(shape))])
    return factor_of


def normal_values(stream_key, shape, deviation, bound, shards=(), held_as=jnp.bfloat16):
    level = level_of(stream_key, shape, shards, -0.22, 0.18) if shards else 1.0
    entries = jax.random.normal(stream_key, shape, jnp.float32) * deviation * level
    return jnp.minimum(jnp.maximum(entries, -bound), bound).astype(held_as)


def setup_inputs(seed: int = 0) -> dict:
    streams_of = jax.random.split(jax.random.key(seed), 7)
    dual_rhs = normal_values(streams_of[0], (SX, SY, SZ, 3, P_SIZE, R), 1.0, 6.0, ((0, 2), (1, 4), (2, 4)), jnp.float32)
    local_flex = draw_local_flex(jax.random.fold_in(streams_of[6], 71), 0)
    corner_coupling = normal_values(streams_of[2], (SX, SY, SZ, 24, Q), (Q // 8) ** -0.5, 0.375, ((0, 2), (1, 4), (2, 4)))
    face_stiffness = draw_face_stiffness(jax.random.fold_in(streams_of[6], 71), 0)
    coarse_inverse = draw_coarse_inverse(jax.random.fold_in(streams_of[6], 71), 0)
    corner_ids = draw_corner_ids(jax.random.fold_in(streams_of[6], 71), 0)
    return {"dual_rhs": dual_rhs, "local_flex": local_flex, "corner_coupling": corner_coupling, "face_stiffness": face_stiffness, "coarse_inverse": coarse_inverse, "corner_ids": corner_ids}


def reference(dual_rhs, local_flex, corner_coupling, face_stiffness, coarse_inverse, corner_ids):
    block_count = SX * SY * SZ
    grid_x = jnp.broadcast_to(jnp.arange(SX)[:, None, None], (SX, SY, SZ))
    grid_y = jnp.broadcast_to(jnp.arange(SY)[None, :, None], (SX, SY, SZ))
    grid_z = jnp.broadcast_to(jnp.arange(SZ)[None, None, :], (SX, SY, SZ))
    face_mask = jnp.stack([grid_x > 0, grid_x < SX - 1, grid_y > 0, grid_y < SY - 1, grid_z > 0, grid_z < SZ - 1], axis=-1).astype(jnp.float32)
    expanded = face_mask[..., None, None]
    face_sign = jnp.array([-1.0, 1.0, -1.0, 1.0, -1.0, 1.0], jnp.float32)[:, None, None]

    def duplicate(owned):
        face_list = []
        for axis_pos in range(3):
            plus_face = owned[:, :, :, axis_pos]
            face_list.append(jnp.roll(plus_face, 1, axis=axis_pos))
            face_list.append(plus_face)
        return jnp.stack(face_list, axis=3) * expanded

    def face_jump(values):
        face_list = []
        for axis_pos in range(3):
            minus_face = values[:, :, :, 2 * axis_pos]
            plus_face = values[:, :, :, 2 * axis_pos + 1]
            face_list.append(jnp.roll(plus_face, 1, axis=axis_pos) - minus_face)
            face_list.append(plus_face - jnp.roll(minus_face, -1, axis=axis_pos))
        return jnp.stack(face_list, axis=3) * expanded

    def face_product(operands):
        return jnp.dot(operands[0], operands[1], preferred_element_type=jnp.float32)

    stiff_flat = face_stiffness.reshape(block_count * 6, P_SIZE, P_SIZE)

    def precondition(dual):
        halved = (0.5 * face_sign * dual).astype(jnp.bfloat16)
        products = lax.map(face_product, (stiff_flat, halved.reshape(block_count * 6, P_SIZE, R)))
        return 0.5 * face_jump(products.reshape(SX, SY, SZ, 6, P_SIZE, R))

    flex_flat = local_flex.reshape(block_count, Q, Q)
    coupling_flat = corner_coupling.reshape(block_count, 24, Q)
    coupling_wide = coupling_flat.astype(jnp.float32)
    id_rows = corner_ids.reshape(block_count, 8)
    dof_ids = jnp.where(id_rows[:, :, None] >= 0, 3 * id_rows[:, :, None] + jnp.arange(3, dtype=jnp.int32)[None, None, :], NC).astype(jnp.int32).reshape(block_count, 24)

    def local_solve(operands):
        flex_block, coupling_block, signed_block = operands
        return (jnp.dot(flex_block, signed_block, preferred_element_type=jnp.float32),
                jnp.dot(coupling_block, signed_block, preferred_element_type=jnp.float32))

    def dual_operator(direction):
        signed = (face_sign * direction).astype(jnp.bfloat16).reshape(block_count, Q, R)
        local_image, corner_part = lax.map(local_solve, (flex_flat, coupling_flat, signed))
        coarse_rhs = jax.ops.segment_sum(corner_part.reshape(block_count * 24, R), dof_ids.reshape(-1), num_segments=NC + 1)[:NC]
        coarse_sol = jnp.dot(coarse_inverse, coarse_rhs.astype(jnp.bfloat16), preferred_element_type=jnp.float32)
        padded = jnp.concatenate([coarse_sol, jnp.zeros((1, R), jnp.float32)], axis=0)
        corner_sol = padded[dof_ids]
        displaced = local_image + jnp.einsum("nkq,nkr->nqr", coupling_wide, corner_sol, precision=lax.Precision.HIGHEST)
        curvature = jnp.sum(signed.astype(jnp.float32) * displaced, axis=(0, 1))
        return face_jump(displaced.reshape(SX, SY, SZ, 6, P_SIZE, R)), curvature

    def inner(left, right):
        return jnp.sum(left[:, :, :, 1::2] * right[:, :, :, 1::2], axis=(0, 1, 2, 3, 4))

    residual = duplicate(dual_rhs)
    multiplier = jnp.zeros_like(residual)
    precond_res = precondition(residual)
    rho_now = inner(residual, precond_res)
    direction = precond_res
    for iteration in range(ITERS):
        image, curvature = dual_operator(direction)
        step_size = rho_now / curvature
        multiplier = multiplier + step_size * direction
        residual = residual - step_size * image
        if iteration + 1 < ITERS:
            precond_res = precondition(residual)
            rho_next = inner(residual, precond_res)
            direction = precond_res + (rho_next / rho_now) * direction
            rho_now = rho_next
    return multiplier[:, :, :, 1::2], residual[:, :, :, 1::2]
```

```python
import functools

import jax
import jax.numpy as jnp
from jax import lax
from jax.experimental import pallas as pl
from jax.experimental.pallas import tpu as pltpu
from jax.sharding import PartitionSpec as P

ITERS = 3
AXES = ("gx", "gy", "gz")
F32 = jnp.float32
BF16 = jnp.bfloat16
MESH = pl.DeviceIdType.MESH


def round_up(value, unit):
    return (value + unit - 1) // unit * unit


def kernel(
    sizes,
    dims,
    rhs_hbm,
    flex_hbm,
    coup_hbm,
    stiff_hbm,
    cinv_hbm,
    ids_ref,
    mult_ref,
    resid_ref,
    rhs_v,
    flex_v,
    coup_v,
    k_own,
    k_nb,
    cinv_v,
    r_send,
    r_recv,
    casm_wide,
    casm_v,
    c_own,
    c_nb,
    corr_v,
    res_v,
    z_v,
    zflat,
    signed_v,
    imgflat,
    img_send,
    img_recv,
    dir_v,
    s_v,
    lam_v,
    coarse_a,
    coarse_b,
    energy_a,
    energy_b,
    local_sem,
    setup_send,
    setup_recv,
    halo_send,
    halo_recv,
    a_send,
    a_recv,
    b_send,
    b_recv,
    ea_send,
    ea_recv,
    eb_send,
    eb_recv,
):
    nx, ny, nz = sizes
    faces, width, cols, ncoarse, corners = dims
    total = faces * width
    ncq = c_own.shape[1]
    wide = c_own.shape[2]
    prow = coarse_a.shape[2]
    here = [lax.axis_index(name) for name in AXES]
    plane = nx * ny
    me_plane = here[0] * ny + here[1]
    has = []
    for axis in range(3):
        has.append(here[axis] > 0)
        has.append(here[axis] < sizes[axis] - 1)
    masks = [jnp.where(flag, 1.0, 0.0).astype(F32) for flag in has]

    def neighbour(face):
        axis = face // 2
        step = 1 if face % 2 else -1
        spot = jnp.clip(here[axis] + step, 0, sizes[axis] - 1)
        return {AXES[axis]: spot}

    def plane_peer(offset):
        index = lax.rem(me_plane + offset, plane)
        return {"gx": index // ny, "gy": lax.rem(index, ny)}

    def z_peer(offset):
        return {"gz": lax.rem(here[2] + offset, nz)}

    loads = []
    for index, (src, dst) in enumerate(
        ((rhs_hbm, rhs_v), (coup_hbm, coup_v), (cinv_hbm, cinv_v), (stiff_hbm, k_own), (flex_hbm, flex_v))
    ):
        copy = pltpu.make_async_copy(src, dst, local_sem.at[index])
        copy.start()
        loads.append(copy)

    for face in range(faces):

        @pl.when(jnp.logical_not(has[face]))
        def _(face=face):
            k_nb[face] = jnp.zeros(k_nb.shape[1:], BF16)
            c_nb[face] = jnp.zeros(c_nb.shape[1:], BF16)
            for it in range(ITERS):
                img_recv[it, face] = jnp.zeros((width, cols), BF16)

    for axis in range(3):

        @pl.when(jnp.logical_not(has[2 * axis]))
        def _(axis=axis):
            r_recv[axis] = jnp.zeros((width, cols), BF16)

    barrier = pltpu.get_barrier_semaphore()
    for offset in range(1, plane):
        pl.semaphore_signal(barrier, inc=1, device_id=plane_peer(offset), device_id_type=MESH)
    for offset in range(1, nz):
        pl.semaphore_signal(barrier, inc=1, device_id=z_peer(offset), device_id_type=MESH)

    loads[0].wait()
    for axis in range(3):
        r_send[axis] = (rhs_v[axis] * masks[2 * axis + 1]).astype(BF16)
    pl.semaphore_wait(barrier, plane - 1 + nz - 1)

    def remote(src, dst, send_sem, recv_sem, target):
        return pltpu.make_async_remote_copy(
            src_ref=src, dst_ref=dst, send_sem=send_sem, recv_sem=recv_sem, device_id=target, device_id_type=MESH
        )

    def rhs_copy(axis):
        return remote(
            r_send.at[axis], r_recv.at[axis], setup_send.at[0, 2 * axis + 1], setup_recv.at[0, 2 * axis],
            neighbour(2 * axis + 1),
        )

    def k_copy(face):
        return remote(
            stiff_hbm.at[face], k_nb.at[face ^ 1], setup_send.at[1, face], setup_recv.at[1, face ^ 1], neighbour(face)
        )

    def c_copy(face):
        return remote(
            c_own.at[face], c_nb.at[face ^ 1], setup_send.at[2, face], setup_recv.at[2, face ^ 1], neighbour(face)
        )

    def halo_copy(it, face):
        return remote(
            img_send.at[it, face], img_recv.at[it, face ^ 1], halo_send.at[it, face], halo_recv.at[it, face ^ 1],
            neighbour(face),
        )

    def when_has(face, action):
        @pl.when(has[face])
        def _():
            action()

    for axis in (2, 0, 1):
        when_has(2 * axis + 1, lambda axis=axis: rhs_copy(axis).start())
    for face in (4, 0, 2, 5, 1, 3):
        when_has(face, lambda face=face: k_copy(face).start())

    loads[1].wait()
    lane = lax.broadcasted_iota(jnp.int32, (1, 3 * corners), 1)
    target_row = jnp.full((1, 3 * corners), -1, jnp.int32)
    for k in range(corners):
        node = ids_ref[k]
        mine = (lane >= 3 * k) & (lane < 3 * k + 3) & (node >= 0)
        target_row = jnp.where(mine, 3 * node + lane - 3 * k, target_row)
    rows = lax.broadcasted_iota(jnp.int32, (ncq, 3 * corners), 0)
    assembly = jnp.where(rows == target_row, 1.0, 0.0).astype(BF16)
    assembled = jnp.dot(assembly, coup_v[...], preferred_element_type=F32)
    casm_v[...] = assembled.astype(BF16)
    casm_wide[...] = jnp.zeros(casm_wide.shape, F32)
    casm_wide[:, 0:total] = assembled
    span = casm_wide.shape[1]
    lanes = lax.broadcasted_iota(jnp.int32, (ncq, wide), 1)
    for face in range(faces):
        start = face * width
        low = start // 128 * 128
        high = min(round_up(start + width, 128), span)
        piece = casm_wide[:, low:high]
        if start > low:
            piece = pltpu.roll(piece, (high - low) - (start - low), 1)
        piece = piece[:, 0:wide]
        c_own[face] = jnp.where(lanes < width, piece, 0.0).astype(BF16)
        when_has(face, lambda face=face: c_copy(face).start())

    for axis in range(3):
        when_has(2 * axis, lambda axis=axis: rhs_copy(axis).wait_recv())
        res_v[2 * axis] = -r_recv[axis].astype(F32)
        res_v[2 * axis + 1] = rhs_v[axis] * masks[2 * axis + 1]
    loads[2].wait()
    loads[3].wait()

    coarse_row = lax.broadcasted_iota(jnp.int32, (prow, cols), 0)
    rho_now = None
    step_size = None
    for it in range(ITERS):
        last = it + 1 == ITERS
        rho_acc = jnp.zeros((1, cols), F32)
        for face in range(faces):
            if it == 0:
                when_has(face, lambda face=face: k_copy(face).wait_send())
                when_has(face, lambda face=face: remote(
                    stiff_hbm.at[face], k_nb.at[face], setup_send.at[1, face], setup_recv.at[1, face], neighbour(face)
                ).wait_recv())
            res = res_v[face]
            half = (0.5 * res).astype(BF16)
            z = jnp.dot(k_own[face], half, preferred_element_type=F32)
            z = z + jnp.dot(k_nb[face], half, preferred_element_type=F32)
            z = z * (0.5 * masks[face])
            z_v[face] = z
            zflat[face * width : (face + 1) * width, :] = z
            if face % 2:
                rho_acc = rho_acc + jnp.sum(res * z, axis=0, keepdims=True)
        signed = zflat[...].astype(BF16)
        signed_v[...] = signed
        if it == 0:
            loads[4].wait()
        coarse_part = jnp.dot(casm_v[...], signed, preferred_element_type=F32)
        if prow > ncq:
            coarse_part = jnp.concatenate([coarse_part, jnp.zeros((prow - ncq, cols), F32)], axis=0)
        coarse_a[it, 0] = jnp.where(coarse_row == ncoarse, rho_acc, coarse_part[0:prow])

        def a_copy(offset, it=it):
            return remote(
                coarse_a.at[it, 0], coarse_a.at[it, offset], a_send.at[it, offset], a_recv.at[it, offset],
                plane_peer(offset),
            )

        def b_copy(offset, it=it):
            return remote(
                coarse_b.at[it, 0], coarse_b.at[it, offset], b_send.at[it, offset], b_recv.at[it, offset],
                z_peer(offset),
            )

        def ea_copy(offset, it=it):
            return remote(
                energy_a.at[it, 0], energy_a.at[it, offset], ea_send.at[it, offset], ea_recv.at[it, offset],
                plane_peer(offset),
            )

        def eb_copy(offset, it=it):
            return remote(
                energy_b.at[it, 0], energy_b.at[it, offset], eb_send.at[it, offset], eb_recv.at[it, offset],
                z_peer(offset),
            )

        for offset in range(1, plane):
            a_copy(offset).start()

        energy_acc = jnp.zeros((8, cols), F32)
        begin = 0
        for face in range(faces):
            end = total if face + 1 == faces else round_up((face + 1) * width, 16)
            image = jnp.dot(flex_v[begin:end, :], signed_v[...], preferred_element_type=F32)
            imgflat[begin:end, :] = image
            weighted = image * signed_v[begin:end, :].astype(F32)
            energy_acc = energy_acc + jnp.sum(weighted.reshape(-1, 8, cols), axis=0)
            begin = end
            img_send[it, face] = imgflat[face * width : (face + 1) * width, :].astype(BF16)
            if not last or face % 2 == 0:
                when_has(face, lambda face=face, it=it: halo_copy(it, face).start())
        energy_a[it, 0] = energy_acc
        for offset in range(1, plane):
            ea_copy(offset).start()

        part = coarse_a[it, 0]
        for offset in range(1, plane):
            a_copy(offset).wait_recv()
            part = part + coarse_a[it, offset]
        coarse_b[it, 0] = part
        for offset in range(1, nz):
            b_copy(offset).start()
        energy = energy_a[it, 0]
        for offset in range(1, plane):
            ea_copy(offset).wait_recv()
            energy = energy + energy_a[it, offset]
        energy_b[it, 0] = energy
        for offset in range(1, nz):
            eb_copy(offset).start()

        if it == 0:
            for face in range(faces):
                when_has(face, lambda face=face: remote(
                    c_own.at[face], c_nb.at[face], setup_send.at[2, face], setup_recv.at[2, face], neighbour(face)
                ).wait_recv())
                own = c_own[face].astype(F32)
                other = c_nb[face].astype(F32)
                stack = jnp.concatenate([own, -other] * (corr_v.shape[2] // (2 * ncq)), axis=0)
                corr_v[face] = stack.T[0:width].astype(BF16)

        coarse = coarse_b[it, 0]
        for offset in range(1, nz):
            b_copy(offset).wait_recv()
            coarse = coarse + coarse_b[it, offset]
        rho = jnp.sum(jnp.where(coarse_row == ncoarse, coarse, 0.0), axis=0, keepdims=True)
        if prow > ncq:
            coarse = coarse[0:ncq]
        elif prow < ncq:
            coarse = jnp.concatenate([coarse, jnp.zeros((ncq - prow, cols), F32)], axis=0)
        rows_q = lax.broadcasted_iota(jnp.int32, (ncq, cols), 0)
        coarse = jnp.where(rows_q < ncoarse, coarse, 0.0)
        sol = jnp.dot(cinv_v[...], coarse[0:ncoarse].astype(BF16), preferred_element_type=F32)
        sol = jnp.concatenate([sol, jnp.zeros((ncq - ncoarse, cols), F32)], axis=0) if ncq > ncoarse else sol
        sol_hi = sol.astype(BF16)
        sol_lo = (sol - sol_hi.astype(F32)).astype(BF16)
        if corr_v.shape[2] == 4 * ncq:
            sol_parts = [jnp.concatenate([sol_hi, sol_hi, sol_lo, sol_lo], axis=0)]
        else:
            sol_parts = [jnp.concatenate([piece, piece], axis=0) for piece in (sol_hi, sol_lo)]
        coarse_energy = jnp.sum(coarse * sol, axis=0, keepdims=True)

        energy = energy_b[it, 0]
        for offset in range(1, nz):
            eb_copy(offset).wait_recv()
            energy = energy + energy_b[it, offset]
        energy = jnp.sum(energy, axis=0, keepdims=True) + coarse_energy

        if it == 0:
            step_size = rho / energy
            beta = None
        else:
            beta = rho / rho_now
            step_size = rho / (energy - beta * rho / step_size)
        rho_now = rho

        for face in range(faces):
            if last and face % 2 == 0:
                continue
            when_has(face, lambda face=face, it=it: remote(
                img_send.at[it, face], img_recv.at[it, face], halo_send.at[it, face], halo_recv.at[it, face],
                neighbour(face),
            ).wait_recv())
            image = img_send[it, face].astype(F32) - img_recv[it, face].astype(F32)
            for piece in sol_parts:
                image = image + jnp.dot(corr_v[face], piece, preferred_element_type=F32)
            image = image * masks[face]
            if it > 0:
                image = image + beta * s_v[face]
            new_res = res_v[face] - step_size * image
            if last:
                resid_ref[face // 2] = new_res
            else:
                s_v[face] = image
                res_v[face] = new_res
            if face % 2:
                axis = face // 2
                direction = z_v[face]
                if it > 0:
                    direction = direction + beta * dir_v[axis]
                if not last:
                    dir_v[axis] = direction
                moved = step_size * direction
                if it > 0:
                    moved = moved + lam_v[axis]
                if last:
                    mult_ref[axis] = moved
                else:
                    lam_v[axis] = moved

    for axis in range(3):
        when_has(2 * axis + 1, lambda axis=axis: rhs_copy(axis).wait_send())
    for face in range(faces):
        when_has(face, lambda face=face: c_copy(face).wait_send())
        for it in range(ITERS):
            if it + 1 < ITERS or face % 2 == 0:
                when_has(face, lambda face=face, it=it: halo_copy(it, face).wait_send())
    for it in range(ITERS):
        for offset in range(1, plane):
            remote(coarse_a.at[it, 0], coarse_a.at[it, offset], a_send.at[it, offset], a_recv.at[it, offset],
                   plane_peer(offset)).wait_send()
            remote(energy_a.at[it, 0], energy_a.at[it, offset], ea_send.at[it, offset], ea_recv.at[it, offset],
                   plane_peer(offset)).wait_send()
        for offset in range(1, nz):
            remote(coarse_b.at[it, 0], coarse_b.at[it, offset], b_send.at[it, offset], b_recv.at[it, offset],
                   z_peer(offset)).wait_send()
            remote(energy_b.at[it, 0], energy_b.at[it, offset], eb_send.at[it, offset], eb_recv.at[it, offset],
                   z_peer(offset)).wait_send()


def body(sizes, dual_rhs, local_flex, corner_coupling, face_stiffness, coarse_inverse, corner_ids):
    rhs = dual_rhs[0, 0, 0]
    flex = local_flex[0, 0, 0]
    coupling = corner_coupling[0, 0, 0]
    stiffness = face_stiffness[0, 0, 0]
    ids = corner_ids[0, 0, 0]
    faces, width, _ = stiffness.shape
    cols = rhs.shape[2]
    ncoarse = coarse_inverse.shape[0]
    corners = ids.shape[0]
    total = faces * width
    ncq = round_up(ncoarse, 32)
    prow = round_up(ncoarse + 1, 8)
    wide = round_up(width, 128)
    span = round_up((faces - 1) * width // 128 * 128 + max(round_up(width + 127, 128), wide), 128)
    nx, ny, nz = sizes
    plane = nx * ny
    dma = pltpu.SemaphoreType.DMA
    any_space = pl.BlockSpec(memory_space=pl.ANY)
    vmem = pl.BlockSpec(memory_space=pltpu.VMEM)
    smem = pl.BlockSpec(memory_space=pltpu.SMEM)
    out = jax.ShapeDtypeStruct(rhs.shape, F32)
    mult, resid = pl.pallas_call(
        functools.partial(kernel, sizes, (faces, width, cols, ncoarse, corners)),
        out_shape=(out, out),
        in_specs=[any_space] * 5 + [smem],
        out_specs=(vmem, vmem),
        scratch_shapes=[
            pltpu.VMEM(rhs.shape, F32),
            pltpu.VMEM(flex.shape, BF16),
            pltpu.VMEM(coupling.shape, BF16),
            pltpu.VMEM(stiffness.shape, BF16),
            pltpu.VMEM(stiffness.shape, BF16),
            pltpu.VMEM(coarse_inverse.shape, BF16),
            pltpu.VMEM((3, width, cols), BF16),
            pltpu.VMEM((3, width, cols), BF16),
            pltpu.VMEM((ncq, span), F32),
            pltpu.VMEM((ncq, total), BF16),
            pltpu.VMEM((faces, ncq, wide), BF16),
            pltpu.VMEM((faces, ncq, wide), BF16),
            pltpu.VMEM((faces, width, (4 if ncq <= 64 else 2) * ncq), BF16),
            pltpu.VMEM((faces, width, cols), F32),
            pltpu.VMEM((faces, width, cols), F32),
            pltpu.VMEM((total, cols), F32),
            pltpu.VMEM((total, cols), BF16),
            pltpu.VMEM((total, cols), F32),
            pltpu.VMEM((ITERS, faces, width, cols), BF16),
            pltpu.VMEM((ITERS, faces, width, cols), BF16),
            pltpu.VMEM((3, width, cols), F32),
            pltpu.VMEM((faces, width, cols), F32),
            pltpu.VMEM((3, width, cols), F32),
            pltpu.VMEM((ITERS, plane, prow, cols), F32),
            pltpu.VMEM((ITERS, nz, prow, cols), F32),
            pltpu.VMEM((ITERS, plane, 8, cols), F32),
            pltpu.VMEM((ITERS, nz, 8, cols), F32),
            dma((5,)),
            dma((3, faces)),
            dma((3, faces)),
            dma((ITERS, faces)),
            dma((ITERS, faces)),
            dma((ITERS, plane)),
            dma((ITERS, plane)),
            dma((ITERS, nz)),
            dma((ITERS, nz)),
            dma((ITERS, plane)),
            dma((ITERS, plane)),
            dma((ITERS, nz)),
            dma((ITERS, nz)),
        ],
        compiler_params=pltpu.CompilerParams(
            collective_id=0, has_side_effects=True, vmem_limit_bytes=62 * 1024 * 1024
        ),
    )(rhs, flex, coupling, stiffness, coarse_inverse, ids)
    return (mult[None, None, None], resid[None, None, None])


def solution(mesh):
    sizes = tuple(mesh.shape[name] for name in AXES)
    placed = (
        P("gx", "gy", "gz", None, None, None),
        P("gx", "gy", "gz", None, None),
        P("gx", "gy", "gz", None, None),
        P("gx", "gy", "gz", None, None, None),
        P(),
        P("gx", "gy", "gz", None),
    )
    return jax.shard_map(
        functools.partial(body, sizes),
        mesh=mesh,
        in_specs=placed,
        out_specs=(P("gx", "gy", "gz", None, None, None), P("gx", "gy", "gz", None, None, None)),
        check_vma=False,
    )
```

```python
import functools

import jax
import jax.numpy as jnp
from jax import lax
from jax.experimental import pallas as pl
from jax.experimental.pallas import tpu as pltpu
from jax.sharding import PartitionSpec as P

ITERS = 3
AXES = ("gx", "gy", "gz")
F32 = jnp.float32
BF16 = jnp.bfloat16
MESH = pl.DeviceIdType.MESH


def round_up(value, unit):
    return (value + unit - 1) // unit * unit


def kernel(
    sizes,
    dims,
    rhs_hbm,
    flex_hbm,
    coup_hbm,
    stiff_hbm,
    cinv_hbm,
    ids_ref,
    mult_ref,
    resid_ref,
    rhs_v,
    flex_v,
    coup_v,
    k_own,
    k_nb,
    cinv_v,
    r_send,
    r_recv,
    casm_wide,
    casm_v,
    c_own,
    c_nb,
    corr_v,
    res_v,
    z_v,
    zflat,
    signed_v,
    imgflat,
    img_send,
    img_recv,
    dir_v,
    s_v,
    lam_v,
    coarse_a,
    coarse_b,
    energy_a,
    energy_b,
    local_sem,
    setup_send,
    setup_recv,
    halo_send,
    halo_recv,
    a_send,
    a_recv,
    b_send,
    b_recv,
    ea_send,
    ea_recv,
    eb_send,
    eb_recv,
):
    nx, ny, nz = sizes
    faces, width, cols, ncoarse, corners = dims
    total = faces * width
    ncq = c_own.shape[1]
    wide = c_own.shape[2]
    here = [lax.axis_index(name) for name in AXES]
    plane = nx * ny
    me_plane = here[0] * ny + here[1]
    has = []
    for axis in range(3):
        has.append(here[axis] > 0)
        has.append(here[axis] < sizes[axis] - 1)
    masks = [jnp.where(flag, 1.0, 0.0).astype(F32) for flag in has]

    def neighbour(face):
        axis = face // 2
        step = 1 if face % 2 else -1
        spot = jnp.clip(here[axis] + step, 0, sizes[axis] - 1)
        return {AXES[axis]: spot}

    def plane_peer(offset):
        index = lax.rem(me_plane + offset, plane)
        return {"gx": index // ny, "gy": lax.rem(index, ny)}

    def z_peer(offset):
        return {"gz": lax.rem(here[2] + offset, nz)}

    barrier = pltpu.get_barrier_semaphore()
    for offset in range(1, plane):
        pl.semaphore_signal(barrier, inc=1, device_id=plane_peer(offset), device_id_type=MESH)
    for offset in range(1, nz):
        pl.semaphore_signal(barrier, inc=1, device_id=z_peer(offset), device_id_type=MESH)

    loads = []
    for index, (src, dst) in enumerate(
        ((rhs_hbm, rhs_v), (coup_hbm, coup_v), (cinv_hbm, cinv_v), (stiff_hbm, k_own), (flex_hbm, flex_v))
    ):
        copy = pltpu.make_async_copy(src, dst, local_sem.at[index])
        copy.start()
        loads.append(copy)

    loads[0].wait()
    for axis in range(3):
        owned = rhs_v[axis, :, 0, :] * masks[2 * axis + 1]
        res_v[2 * axis + 1] = owned
        r_send[axis] = owned.astype(BF16)
    pl.semaphore_wait(barrier, plane - 1 + nz - 1)

    def remote(src, dst, send_sem, recv_sem, target):
        return pltpu.make_async_remote_copy(
            src_ref=src, dst_ref=dst, send_sem=send_sem, recv_sem=recv_sem, device_id=target, device_id_type=MESH
        )

    def rhs_copy(axis):
        return remote(
            r_send.at[axis], r_recv.at[axis], setup_send.at[0, 2 * axis + 1], setup_recv.at[0, 2 * axis],
            neighbour(2 * axis + 1),
        )

    def k_copy(face):
        return remote(
            k_own.at[face], k_nb.at[face ^ 1], setup_send.at[1, face], setup_recv.at[1, face ^ 1], neighbour(face)
        )

    def c_copy(face):
        return remote(
            c_own.at[face], c_nb.at[face ^ 1], setup_send.at[2, face], setup_recv.at[2, face ^ 1], neighbour(face)
        )

    def halo_copy(it, face):
        return remote(
            img_send.at[it, face], img_recv.at[it, face ^ 1], halo_send.at[it, face], halo_recv.at[it, face ^ 1],
            neighbour(face),
        )

    def when_has(face, action):
        @pl.when(has[face])
        def _():
            action()

    for axis in (2, 0, 1):
        when_has(2 * axis + 1, lambda axis=axis: rhs_copy(axis).start())
    loads[3].wait()
    for face in (4, 0, 2, 5, 1, 3):
        when_has(face, lambda face=face: k_copy(face).start())

    for face in range(faces):

        @pl.when(jnp.logical_not(has[face]))
        def _(face=face):
            k_nb[face] = jnp.zeros(k_nb.shape[1:], BF16)
            c_nb[face] = jnp.zeros(c_nb.shape[1:], BF16)
            for it in range(ITERS):
                img_recv[it, face] = jnp.zeros((width, cols), BF16)

    for axis in range(3):

        @pl.when(jnp.logical_not(has[2 * axis]))
        def _(axis=axis):
            r_recv[axis] = jnp.zeros((width, cols), BF16)

    loads[1].wait()
    lane = lax.broadcasted_iota(jnp.int32, (1, 3 * corners), 1)
    target_row = jnp.full((1, 3 * corners), -1, jnp.int32)
    for k in range(corners):
        node = ids_ref[k]
        mine = (lane >= 3 * k) & (lane < 3 * k + 3) & (node >= 0)
        target_row = jnp.where(mine, 3 * node + lane - 3 * k, target_row)
    rows = lax.broadcasted_iota(jnp.int32, (ncq, 3 * corners), 0)
    assembly = jnp.where(rows == target_row, 1.0, 0.0).astype(BF16)
    assembled = jnp.dot(assembly, coup_v[...], preferred_element_type=F32)
    casm_v[...] = assembled.astype(BF16)
    casm_wide[...] = jnp.zeros(casm_wide.shape, F32)
    casm_wide[:, 0:total] = assembled
    span = casm_wide.shape[1]
    lanes = lax.broadcasted_iota(jnp.int32, (ncq, wide), 1)
    for face in range(faces):
        start = face * width
        low = start // 128 * 128
        high = min(round_up(start + width, 128), span)
        piece = casm_wide[:, low:high]
        if start > low:
            piece = pltpu.roll(piece, (high - low) - (start - low), 1)
        piece = piece[:, 0:wide]
        c_own[face] = jnp.where(lanes < width, piece, 0.0).astype(BF16)
        when_has(face, lambda face=face: c_copy(face).start())

    for axis in range(3):
        when_has(2 * axis, lambda axis=axis: rhs_copy(axis).wait_recv())
        res_v[2 * axis] = -r_recv[axis].astype(F32)
    loads[2].wait()

    scalar_row = lax.broadcasted_iota(jnp.int32, (8, cols), 0)
    rho_now = None
    step_size = None
    for it in range(ITERS):
        last = it + 1 == ITERS
        rho_acc = jnp.zeros((1, cols), F32)
        if it == 0:
            for face in range(faces):
                when_has(face, lambda face=face: remote(
                    k_own.at[face], k_nb.at[face], setup_send.at[1, face], setup_recv.at[1, face], neighbour(face)
                ).wait_recv())
        for face in range(faces):
            res = res_v[face]
            half = (0.5 * res).astype(BF16)
            z = jnp.dot(k_own[face], half, preferred_element_type=F32)
            z = z + jnp.dot(k_nb[face], half, preferred_element_type=F32)
            z = z * (0.5 * masks[face])
            z_v[face] = z
            zflat[face * width : (face + 1) * width, :] = z
            if face % 2:
                rho_acc = rho_acc + jnp.sum(res * z, axis=0, keepdims=True)
        signed = zflat[...].astype(BF16)
        signed_v[...] = signed
        if it == 0:
            loads[4].wait()
        coarse_part = jnp.dot(casm_v[...], signed, preferred_element_type=F32)
        coarse_a[it, 0] = coarse_part.astype(BF16)

        def a_copy(offset, it=it):
            return remote(
                coarse_a.at[it, 0], coarse_a.at[it, offset], a_send.at[it, offset], a_recv.at[it, offset],
                plane_peer(offset),
            )

        def b_copy(offset, it=it):
            return remote(
                coarse_b.at[it, 0], coarse_b.at[it, offset], b_send.at[it, offset], b_recv.at[it, offset],
                z_peer(offset),
            )

        def ea_copy(offset, it=it):
            return remote(
                energy_a.at[it, 0], energy_a.at[it, offset], ea_send.at[it, offset], ea_recv.at[it, offset],
                plane_peer(offset),
            )

        def eb_copy(offset, it=it):
            return remote(
                energy_b.at[it, 0], energy_b.at[it, offset], eb_send.at[it, offset], eb_recv.at[it, offset],
                z_peer(offset),
            )

        for offset in range(1, plane):
            a_copy(offset).start()

        energy_acc = jnp.zeros((8, cols), F32)
        cuts = [0] + [round_up(2 * a * width, 16) for a in range(1, faces // 2)] + [total]
        order = [faces // 2 - 1] + list(range(faces // 2 - 1))
        for position, axis in enumerate(order):
            begin, end = cuts[axis], cuts[axis + 1]
            image = jnp.dot(flex_v[begin:end, :], signed_v[...], preferred_element_type=F32)
            imgflat[begin:end, :] = image
            weighted = image * signed_v[begin:end, :].astype(F32)
            energy_acc = energy_acc + jnp.sum(weighted.reshape(-1, 8, cols), axis=0)
            for face in (2 * axis, 2 * axis + 1):
                img_send[it, face] = imgflat[face * width : (face + 1) * width, :].astype(BF16)
            for face in (2 * axis, 2 * axis + 1):
                if not last or face % 2 == 0:
                    when_has(face, lambda face=face, it=it: halo_copy(it, face).start())
        energy_row = jnp.sum(energy_acc, axis=0, keepdims=True)
        energy_a[it, 0] = jnp.where(scalar_row == 0, energy_row, jnp.where(scalar_row == 1, rho_acc, 0.0))
        for offset in range(1, plane):
            ea_copy(offset).start()

        part = coarse_a[it, 0].astype(F32)
        for offset in range(1, plane):
            a_copy(offset).wait_recv()
            part = part + coarse_a[it, offset].astype(F32)
        coarse_b[it, 0] = part.astype(BF16)
        for offset in range(1, nz):
            b_copy(offset).start()
        energy = energy_a[it, 0]
        for offset in range(1, plane):
            ea_copy(offset).wait_recv()
            energy = energy + energy_a[it, offset]
        energy_b[it, 0] = energy
        for offset in range(1, nz):
            eb_copy(offset).start()

        if it == 0:
            for face in range(faces):
                when_has(face, lambda face=face: remote(
                    c_own.at[face], c_nb.at[face], setup_send.at[2, face], setup_recv.at[2, face], neighbour(face)
                ).wait_recv())
                own = c_own[face].astype(F32)
                other = c_nb[face].astype(F32)
                stack = jnp.concatenate([own, -other] * (corr_v.shape[2] // (2 * ncq)), axis=0)
                corr_v[face] = stack.T[0:width].astype(BF16)

        coarse = part
        for offset in range(1, nz):
            b_copy(offset).wait_recv()
            coarse = coarse + coarse_b[it, offset].astype(F32)
        sol = jnp.dot(cinv_v[...], coarse[0:ncoarse].astype(BF16), preferred_element_type=F32)
        sol = jnp.concatenate([sol, jnp.zeros((ncq - ncoarse, cols), F32)], axis=0) if ncq > ncoarse else sol
        sol_hi = sol.astype(BF16)
        sol_lo = (sol - sol_hi.astype(F32)).astype(BF16)
        if corr_v.shape[2] == 4 * ncq:
            sol_parts = [jnp.concatenate([sol_hi, sol_hi, sol_lo, sol_lo], axis=0)]
        else:
            sol_parts = [jnp.concatenate([piece, piece], axis=0) for piece in (sol_hi, sol_lo)]
        coarse_energy = jnp.sum(coarse * sol, axis=0, keepdims=True)

        energy = energy_b[it, 0]
        for offset in range(1, nz):
            eb_copy(offset).wait_recv()
            energy = energy + energy_b[it, offset]
        rho = energy[1:2]
        energy = energy[0:1] + coarse_energy

        if it == 0:
            step_size = rho / energy
            beta = None
        else:
            beta = rho / rho_now
            step_size = rho / (energy - beta * rho / step_size)
        rho_now = rho

        for face in range(faces):
            if last and face % 2 == 0:
                continue
            when_has(face, lambda face=face, it=it: remote(
                img_send.at[it, face], img_recv.at[it, face], halo_send.at[it, face], halo_recv.at[it, face],
                neighbour(face),
            ).wait_recv())
        for face in range(faces):
            if last and face % 2 == 0:
                continue
            image = img_send[it, face].astype(F32) - img_recv[it, face].astype(F32)
            for piece in sol_parts:
                image = image + jnp.dot(corr_v[face], piece, preferred_element_type=F32)
            image = image * masks[face]
            if it > 0:
                image = image + beta * s_v[face]
            new_res = res_v[face] - step_size * image
            if last:
                resid_ref[face // 2, :, 0, :] = new_res
            else:
                s_v[face] = image
                res_v[face] = new_res
            if face % 2:
                axis = face // 2
                direction = z_v[face]
                if it > 0:
                    direction = direction + beta * dir_v[axis]
                if not last:
                    dir_v[axis] = direction
                moved = step_size * direction
                if it > 0:
                    moved = moved + lam_v[axis]
                if last:
                    mult_ref[axis, :, 0, :] = moved
                else:
                    lam_v[axis] = moved

    for axis in range(3):
        when_has(2 * axis + 1, lambda axis=axis: rhs_copy(axis).wait_send())
    for face in range(faces):
        when_has(face, lambda face=face: k_copy(face).wait_send())
        when_has(face, lambda face=face: c_copy(face).wait_send())
        for it in range(ITERS):
            if it + 1 < ITERS or face % 2 == 0:
                when_has(face, lambda face=face, it=it: halo_copy(it, face).wait_send())
    for it in range(ITERS):
        for offset in range(1, plane):
            remote(coarse_a.at[it, 0], coarse_a.at[it, offset], a_send.at[it, offset], a_recv.at[it, offset],
                   plane_peer(offset)).wait_send()
            remote(energy_a.at[it, 0], energy_a.at[it, offset], ea_send.at[it, offset], ea_recv.at[it, offset],
                   plane_peer(offset)).wait_send()
        for offset in range(1, nz):
            remote(coarse_b.at[it, 0], coarse_b.at[it, offset], b_send.at[it, offset], b_recv.at[it, offset],
                   z_peer(offset)).wait_send()
            remote(energy_b.at[it, 0], energy_b.at[it, offset], eb_send.at[it, offset], eb_recv.at[it, offset],
                   z_peer(offset)).wait_send()


def body(sizes, dual_rhs, local_flex, corner_coupling, face_stiffness, coarse_inverse, corner_ids):
    rhs = dual_rhs.reshape(dual_rhs.shape[3:5] + (1,) + dual_rhs.shape[5:])
    flex = local_flex[0, 0, 0]
    coupling = corner_coupling[0, 0, 0]
    stiffness = face_stiffness[0, 0, 0]
    ids = corner_ids[0, 0, 0]
    faces, width, _ = stiffness.shape
    cols = rhs.shape[3]
    ncoarse = coarse_inverse.shape[0]
    corners = ids.shape[0]
    total = faces * width
    ncq = round_up(ncoarse, 32)
    wide = round_up(width, 128)
    span = round_up((faces - 1) * width // 128 * 128 + max(round_up(width + 127, 128), wide), 128)
    nx, ny, nz = sizes
    plane = nx * ny
    dma = pltpu.SemaphoreType.DMA
    any_space = pl.BlockSpec(memory_space=pl.ANY)
    vmem = pl.BlockSpec(memory_space=pltpu.VMEM)
    smem = pl.BlockSpec(memory_space=pltpu.SMEM)
    out = jax.ShapeDtypeStruct(rhs.shape, F32)
    mult, resid = pl.pallas_call(
        functools.partial(kernel, sizes, (faces, width, cols, ncoarse, corners)),
        out_shape=(out, out),
        in_specs=[any_space] * 5 + [smem],
        out_specs=(vmem, vmem),
        scratch_shapes=[
            pltpu.VMEM(rhs.shape, F32),
            pltpu.VMEM(flex.shape, BF16),
            pltpu.VMEM(coupling.shape, BF16),
            pltpu.VMEM(stiffness.shape, BF16),
            pltpu.VMEM(stiffness.shape, BF16),
            pltpu.VMEM(coarse_inverse.shape, BF16),
            pltpu.VMEM((3, width, cols), BF16),
            pltpu.VMEM((3, width, cols), BF16),
            pltpu.VMEM((ncq, span), F32),
            pltpu.VMEM((ncq, total), BF16),
            pltpu.VMEM((faces, ncq, wide), BF16),
            pltpu.VMEM((faces, ncq, wide), BF16),
            pltpu.VMEM((faces, width, (4 if ncq <= 64 else 2) * ncq), BF16),
            pltpu.VMEM((faces, width, cols), F32),
            pltpu.VMEM((faces, width, cols), F32),
            pltpu.VMEM((total, cols), F32),
            pltpu.VMEM((total, cols), BF16),
            pltpu.VMEM((total, cols), F32),
            pltpu.VMEM((ITERS, faces, width, cols), BF16),
            pltpu.VMEM((ITERS, faces, width, cols), BF16),
            pltpu.VMEM((3, width, cols), F32),
            pltpu.VMEM((faces, width, cols), F32),
            pltpu.VMEM((3, width, cols), F32),
            pltpu.VMEM((ITERS, plane, ncq, cols), BF16),
            pltpu.VMEM((ITERS, nz, ncq, cols), BF16),
            pltpu.VMEM((ITERS, plane, 8, cols), F32),
            pltpu.VMEM((ITERS, nz, 8, cols), F32),
            dma((5,)),
            dma((3, faces)),
            dma((3, faces)),
            dma((ITERS, faces)),
            dma((ITERS, faces)),
            dma((ITERS, plane)),
            dma((ITERS, plane)),
            dma((ITERS, nz)),
            dma((ITERS, nz)),
            dma((ITERS, plane)),
            dma((ITERS, plane)),
            dma((ITERS, nz)),
            dma((ITERS, nz)),
        ],
        compiler_params=pltpu.CompilerParams(
            collective_id=0, has_side_effects=True, vmem_limit_bytes=62 * 1024 * 1024
        ),
    )(rhs, flex, coupling, stiffness, coarse_inverse, ids)
    return (mult.reshape(dual_rhs.shape), resid.reshape(dual_rhs.shape))


def solution(mesh):
    sizes = tuple(mesh.shape[name] for name in AXES)
    placed = (
        P("gx", "gy", "gz", None, None, None),
        P("gx", "gy", "gz", None, None),
        P("gx", "gy", "gz", None, None),
        P("gx", "gy", "gz", None, None, None),
        P(),
        P("gx", "gy", "gz", None),
    )
    return jax.shard_map(
        functools.partial(body, sizes),
        mesh=mesh,
        in_specs=placed,
        out_specs=(P("gx", "gy", "gz", None, None, None), P("gx", "gy", "gz", None, None, None)),
        check_vma=False,
    )
```
